32 devices in a mesh: rep: 1 (over z), dp: 32 (over x, y, core).
Axes of the slice: x: 4, y: 4, z: 1, core: 2. Of those that a mesh axis runs over, the one named last changes fastest.
The devices are a block of a 4x4x8 slice.
Arguments:
- a: bfloat16 [32, 2, 4096, 896], P(('rep', 'dp'))
- g: bfloat16 [32, 2, 4096, 2304], P(('rep', 'dp'))
Outputs:
- output: bfloat16 [2, 896, 2304], P('rep')
All inputs are finite; a program needn't handle non-finite values.
Results may differ from the reference program's by a relative error of at most 0.012.
Values are sent between devices in bfloat16 or wider.
A program may use at most 768 MiB of HBM per device.

```python
import jax
import jax.numpy as jnp
from jax import lax

DEVICES = 32
MATRICES = 2
TOKENS = 4096
D = 896
FF = 2304


def setup_inputs(seed: int = 0, part: int = 0) -> dict:
    ka, kg, ks = (jax.random.fold_in(k, part) for k in jax.random.split(jax.random.key(seed), 3))
    size = 2.0 ** jax.random.uniform(ks, (DEVICES, MATRICES, 1, 1), jnp.float32, -1.0, 1.0)
    a = jax.random.normal(ka, (DEVICES, MATRICES, TOKENS, D), jnp.float32)
    g = size * jax.random.normal(kg, (DEVICES, MATRICES, TOKENS, FF), jnp.float32) * (DEVICES * TOKENS) ** -0.5
    return {"a": a.astype(jnp.bfloat16), "g": g.astype(jnp.bfloat16)}


def reference(a, g):
    def take(so_far, one):
        return so_far + jnp.einsum("ntd,ntf->ndf", *one, preferred_element_type=jnp.float32), None

    return lax.scan(take, jnp.zeros((MATRICES, D, FF), jnp.float32), (a, g))[0].astype(jnp.bfloat16)
```

```python
import functools
import math

import jax
import jax.numpy as jnp
from jax import lax
from jax.experimental import pallas as pl
from jax.experimental.pallas import tpu as pltpu
from jax.sharding import PartitionSpec as P

BF, F32 = jnp.bfloat16, jnp.float32
W = 128
HEAD = 3
TB = 512
TB1 = 1024
LAG = dict(A=0, B=1, C=3, D=5, E=7, F=9, G=11, H=13, I=15, J=17, L=19)
RING = 5


def kernel(n, mats, tokens, rows, cols, a_ref, g_ref, o_ref,
           at, ast, gb, gh, acc, xs, xr, cs, sb, rb, ps, tb, ub,
           asem, gsem, ss, rs):
    side = math.isqrt(n // 2)
    per = cols // (2 * W)
    K = mats * per
    me = lax.axis_index("dp")
    c = lax.rem(me, 2)
    y = lax.rem(me // 2, side)
    x = me // (2 * side)
    p = x * (1 - c) + y * c
    q = y * (1 - c) + x * c

    def dev(p_, q_, c_):
        x_ = p_ * (1 - c) + q_ * c
        y_ = q_ * (1 - c) + p_ * c
        return (x_ * side + y_) * 2 + c_

    def at_pos(v, d):
        return lax.rem(v + d + side, side)

    partner = dev(p, q, 1 - c)

    def remote(i, k, src, dst, to):
        return pltpu.make_async_remote_copy(
            src_ref=src, dst_ref=dst, send_sem=ss.at[i, k], recv_sem=rs.at[i, k],
            device_id={"dp": to}, device_id_type=pl.DeviceIdType.MESH)

    def send(i, k, src, dst, to):
        remote(i, k, src, dst, to).start()

    def recv(i, k, dst):
        remote(i, k, dst, dst, partner).wait_recv()

    def sent(i, k, src):
        remote(i, k, src, src, partner).wait_send()

    def dirs(k):
        d = 1 - 2 * lax.rem(k, 2)
        return d

    def stage_a(k):
        xs[k] = acc[lax.rem(k, 4), 1 - c].astype(BF)
        send(0, k, xs.at[k], xr.at[k], partner)

    def stage_b(k):
        d = dirs(k)
        f, b, o = at_pos(p, d), at_pos(p, -d), at_pos(p, 2)
        recv(0, k, xr.at[k])
        s = lax.rem(k, RING)

        def part(i):
            r = pl.ds(pl.multiple_of(i * (rows // side), rows // side), rows // side)
            return acc[lax.rem(k, 4), c, r, :] + xr[k, r, :].astype(F32)

        sb[k, 0] = part(o).astype(BF)
        send(1, k, sb.at[k, 0], rb.at[k, 0], dev(f, q, c))
        sb[k, 1] = part(b).astype(BF)
        send(2, k, sb.at[k, 1], rb.at[k, 1], dev(b, q, c))
        cs[s, 0] = part(f)
        cs[s, 1] = part(p)

    def stage_c(k):
        d = dirs(k)
        s = lax.rem(k, RING)
        recv(1, k, rb.at[k, 0])
        sb[k, 2] = (cs[s, 0] + rb[k, 0].astype(F32)).astype(BF)
        send(3, k, sb.at[k, 2], rb.at[k, 2], dev(at_pos(p, d), q, c))

    def stage_d(k):
        d = dirs(k)
        s = lax.rem(k, RING)
        f, b, o = at_pos(q, d), at_pos(q, -d), at_pos(q, 2)
        recv(2, k, rb.at[k, 1])
        recv(3, k, rb.at[k, 2])
        tot = cs[s, 1] + rb[k, 1].astype(F32) + rb[k, 2].astype(F32)
        ps[s] = tot.reshape(ps.shape[1:])
        tb[k, 0] = ps[s, o].astype(BF)
        send(4, k, tb.at[k, 0], ub.at[k, 0], dev(p, f, c))
        tb[k, 1] = ps[s, b].astype(BF)
        send(5, k, tb.at[k, 1], ub.at[k, 1], dev(p, b, c))

    def stage_e(k):
        f = at_pos(q, dirs(k))
        s = lax.rem(k, RING)
        recv(4, k, ub.at[k, 0])
        tb[k, 2] = (ps[s, f] + ub[k, 0].astype(F32)).astype(BF)
        send(6, k, tb.at[k, 2], ub.at[k, 2], dev(p, f, c))

    def stage_f(k):
        d = dirs(k)
        s = lax.rem(k, RING)
        recv(5, k, ub.at[k, 1])
        recv(6, k, ub.at[k, 2])
        o_ref[k, c, p, q] = (ps[s, q] + ub[k, 1].astype(F32) + ub[k, 2].astype(F32)).astype(BF)
        mine = o_ref.at[k, c, p, q]
        send(7, k, mine, mine, dev(p, at_pos(q, d), c))
        send(8, k, mine, mine, dev(p, at_pos(q, -d), c))

    def stage_g(k):
        d = dirs(k)
        piece = o_ref.at[k, c, p, at_pos(q, -d)]
        recv(7, k, piece)
        send(9, k, piece, piece, dev(p, at_pos(q, d), c))

    def stage_h(k):
        d = dirs(k)
        recv(8, k, o_ref.at[k, c, p, at_pos(q, d)])
        recv(9, k, o_ref.at[k, c, p, at_pos(q, 2)])
        mine = o_ref.at[k, c, p]
        send(10, k, mine, mine, dev(at_pos(p, d), q, c))
        send(11, k, mine, mine, dev(at_pos(p, -d), q, c))
        send(13, k, mine, mine, partner)

    def stage_i(k):
        d = dirs(k)
        piece = o_ref.at[k, c, at_pos(p, -d)]
        recv(10, k, piece)
        send(12, k, piece, piece, dev(at_pos(p, d), q, c))
        send(14, k, piece, piece, partner)
        piece = o_ref.at[k, c, at_pos(p, d)]
        recv(11, k, piece)
        send(15, k, piece, piece, partner)

    def stage_j(k):
        piece = o_ref.at[k, c, at_pos(p, 2)]
        recv(12, k, piece)
        send(16, k, piece, piece, partner)

    def stage_l(k):
        d = dirs(k)
        for i, v in ((13, 0), (14, -d), (15, d), (16, 2)):
            recv(i, k, o_ref.at[k, 1 - c, at_pos(q, v)])
        sent(0, k, xs.at[k])
        for i in range(3):
            sent(1 + i, k, sb.at[k, i])
            sent(4 + i, k, tb.at[k, i])
        sent(7, k, o_ref.at[k, c, p, q])
        sent(8, k, o_ref.at[k, c, p, q])
        sent(9, k, o_ref.at[k, c, p, at_pos(q, -d)])
        sent(10, k, o_ref.at[k, c, p])
        sent(11, k, o_ref.at[k, c, p])
        sent(12, k, o_ref.at[k, c, at_pos(p, -d)])
        sent(13, k, o_ref.at[k, c, p])
        sent(14, k, o_ref.at[k, c, at_pos(p, -d)])
        sent(15, k, o_ref.at[k, c, at_pos(p, d)])
        sent(16, k, o_ref.at[k, c, at_pos(p, 2)])

    stages = [("A", stage_a), ("L", stage_l), ("J", stage_j), ("I", stage_i), ("H", stage_h), ("G", stage_g),
              ("F", stage_f), ("E", stage_e), ("D", stage_d), ("C", stage_c), ("B", stage_b)]

    def service(t, lo, hi):
        for name, fn in stages:
            lag = LAG[name]
            if hi - 1 - lag < 0 or lo - lag >= K:
                continue
            if lo - lag >= 0 and hi - 1 - lag < K:
                fn(t - lag)
            else:
                pl.when((t >= lag) & (t < K + lag))(functools.partial(fn, t - lag))

    def steps(lo, hi, body):
        def run(t, _):
            body(t)
            service(t, lo, hi)
            return 0
        lax.fori_loop(lo, hi, run, 0)

    barrier = pltpu.get_barrier_semaphore()
    for to in (partner, dev(at_pos(p, 1), q, c), dev(at_pos(p, -1), q, c),
               dev(p, at_pos(q, 1), c), dev(p, at_pos(q, -1), c)):
        pl.semaphore_signal(barrier, inc=1, device_id={"dp": to}, device_id_type=pl.DeviceIdType.MESH)

    def gcopy(k):
        s = lax.rem(k, 2)
        return pltpu.make_async_copy(
            g_ref.at[0, k // per, :, pl.ds(pl.multiple_of(lax.rem(k, per) * 2 * W, 2 * W), 2 * W)], gb.at[s], gsem.at[s])

    def ghead(b):
        s = lax.rem(b, 2)
        return pltpu.make_async_copy(
            g_ref.at[0, 0, pl.ds(pl.multiple_of(b * TB, TB), TB), pl.ds(0, HEAD * 2 * W)], gh.at[s], gsem.at[s])

    def acopy(m, b, size):
        s = lax.rem(b, 2)
        return pltpu.make_async_copy(
            a_ref.at[0, m, pl.ds(pl.multiple_of(b * size, size), size), :], ast.at[s, pl.ds(0, size)], asem.at[s])

    nb = tokens // TB
    acopy(0, 0, TB).start()
    ghead(0).start()
    acc[0:HEAD] = jnp.zeros_like(acc[0:HEAD])

    def head(b, _):
        s = lax.rem(b, 2)
        @pl.when(b + 1 < nb)
        def _():
            acopy(0, b + 1, TB).start()
            ghead(b + 1).start()
        acopy(0, b, TB).wait()
        ghead(b).wait()
        t = ast[s, 0:TB].T
        at[0, :, pl.ds(pl.multiple_of(b * TB, TB), TB)] = t
        res = jnp.dot(t, gh[s], preferred_element_type=F32)
        for h in range(HEAD):
            for i in range(2):
                acc[h, i] += res[:, (2 * h + i) * W:(2 * h + i + 1) * W]
        return 0

    lax.fori_loop(0, nb, head, 0)
    acopy(1, 0, TB1).start()
    gcopy(HEAD).start()
    pl.semaphore_wait(barrier, 5)

    def compute(t, m):
        s = lax.rem(t, 2)
        res = jnp.dot(at[m], gb[s], preferred_element_type=F32)
        acc[lax.rem(t, 4), 0] = res[:, :W]
        acc[lax.rem(t, 4), 1] = res[:, W:]

    def with_transpose(t):
        s = lax.rem(t, 2)
        b = t - HEAD
        gcopy(t + 1).start()
        @pl.when(b + 1 < tokens // TB1)
        def _():
            acopy(1, b + 1, TB1).start()
        acopy(1, b, TB1).wait()
        gcopy(t).wait()
        at[1, :, pl.ds(pl.multiple_of(b * TB1, TB1), TB1)] = ast[lax.rem(b, 2)].T
        compute(t, 0)

    def plain(t):
        @pl.when(t + 1 < K)
        def _():
            gcopy(t + 1).start()
        gcopy(t).wait()
        compute(t, t // per)

    for t in range(HEAD):
        service(t, t, t + 1)
    mid = HEAD + tokens // TB1
    steps(HEAD, mid, with_transpose)
    steps(mid, K, plain)
    steps(K, K + LAG["L"], lambda t: None)


def write(o_ref, out_ref, sem):
    blocks, rows, w = o_ref.shape
    per = blocks // out_ref.shape[0]

    def copy(k):
        return pltpu.make_async_copy(
            o_ref.at[k], out_ref.at[k // per, :, pl.ds(k % per * w, w)], sem.at[k])

    for k in range(blocks):
        copy(k).start()
    for k in range(blocks):
        copy(k).wait()


def solution(mesh):
    n = mesh.shape["dp"]
    side = math.isqrt(n // 2)

    def step(a, g):
        _, mats, tokens, rows = a.shape
        cols = g.shape[-1]
        K = mats * cols // (2 * W)
        quarter, piece = rows // side, rows // side // side
        o = pl.pallas_call(
            functools.partial(kernel, n, mats, tokens, rows, cols),
            out_shape=pltpu.VMEM((K, 2, side, side, piece, W), BF),
            in_specs=[pl.BlockSpec(memory_space=pl.ANY)] * 2,
            out_specs=pl.BlockSpec(memory_space=pltpu.VMEM),
            scratch_shapes=[
                pltpu.VMEM((mats, rows, tokens), BF),
                pltpu.VMEM((2, TB1, rows), BF),
                pltpu.VMEM((2, tokens, 2 * W), BF),
                pltpu.VMEM((2, TB, HEAD * 2 * W), BF),
                pltpu.VMEM((4, 2, rows, W), F32),
                pltpu.VMEM((K, rows, W), BF),
                pltpu.VMEM((K, rows, W), BF),
                pltpu.VMEM((RING, 2, quarter, W), F32),
                pltpu.VMEM((K, 3, quarter, W), BF),
                pltpu.VMEM((K, 3, quarter, W), BF),
                pltpu.VMEM((RING, side, piece, W), F32),
                pltpu.VMEM((K, 3, piece, W), BF),
                pltpu.VMEM((K, 3, piece, W), BF),
                pltpu.SemaphoreType.DMA((2,)),
                pltpu.SemaphoreType.DMA((2,)),
                pltpu.SemaphoreType.DMA((17, K)),
                pltpu.SemaphoreType.DMA((17, K)),
            ],
            name="sums",
            compiler_params=pltpu.CompilerParams(
                collective_id=0, has_side_effects=True, vmem_limit_bytes=54 * 2**20),
        )(a, g)
        o = o.reshape(K * 2, rows, W)
        return pl.pallas_call(
            write,
            out_shape=jax.ShapeDtypeStruct((mats, rows, cols), BF),
            in_specs=[pl.BlockSpec(memory_space=pltpu.VMEM)],
            out_specs=pl.BlockSpec(memory_space=pl.ANY),
            scratch_shapes=[pltpu.SemaphoreType.DMA((K * 2,))],
            name="write",
            compiler_params=pltpu.CompilerParams(vmem_limit_bytes=8 * 2**20),
        )(pltpu.with_memory_space_constraint(o, pltpu.VMEM))

    return jax.shard_map(
        step, mesh=mesh, in_specs=(P(("rep", "dp")), P(("rep", "dp"))), out_specs=P("rep"), check_vma=False)
```

```python
import functools
import math

import jax
import jax.numpy as jnp
from jax import lax
from jax.experimental import pallas as pl
from jax.experimental.pallas import tpu as pltpu
from jax.sharding import PartitionSpec as P

BF, F32 = jnp.bfloat16, jnp.float32
W = 128
TB = 512
RING = 4
KINDS = "ABCDFHIP"
SLOTS = 6
DIRECT, SPREAD, FUSED = (0, 1, 2, 3, 15, 16, 17,), (16, 17,), ()
STEPS = (
    (),
    (),
    ("b0",),
    ("b1",),
    (),
    ("b2", "B3",),
    ("d0", "b4", "d1",),
    ("b5", "d3",),
    ("d2", "B6",),
    ("c4", "B7", "f0", "f1",),
    ("c6", "f3", "b8", "C5",),
    ("B9", "c7", "f2",),
    ("d4", "B10", "d5", "H0", "H1",),
    ("B11", "C9", "C8", "H3", "d6",),
    ("H2", "B12", "d7", "C10",),
    ("F4", "F5", "I0", "D8", "c11", "B13", "I1",),
    ("C12", "D9", "B14", "F6", "I2", "B15", "I3",),
    ("C13", "D11", "D10", "H5", "D12", "C14", "F8", "F7", "b16", "H4",),
)
DRAIN = (
    "F11", "D15", "D14", "D13", "B17", "F12", "F9", "D16", "H6", "I4", "J1", "J2", "I5", "F15", "H11", "F14", "F10",
    "H7", "H9", "H8", "D17", "F16", "H15", "J0", "J4", "F13", "L2", "H12", "H10", "H14", "I6", "I9", "F17", "I8", "I7",
    "J3", "H13", "I15", "H16", "I14", "I10", "I11", "H17", "J15", "I13", "J8", "I12", "J7", "L1", "J10", "J16", "L15",
    "J11", "J9", "J14", "L9", "L4", "J5", "J17", "L10", "L11", "L16", "L3", "L7", "L14", "L8", "J13", "J6", "J12",
    "L17", "L0", "L5", "L6", "L13", "L12",
)


def kernel(n, mats, tokens, rows, cols, a_ref, g_ref, o_ref,
           at, ast, gb, acc, xs, xr, cs, sb, rb, ps, tb, ub, fr,
           asem, gsem, ss, rs):
    side = math.isqrt(n // 2)
    per = cols // (2 * W)
    K = mats * per
    me = lax.axis_index("dp")
    c = lax.rem(me, 2)
    y = lax.rem(me // 2, side)
    x = me // (2 * side)
    p = x * (1 - c) + y * c
    q = y * (1 - c) + x * c

    def dev(p_, q_, c_):
        x_ = p_ * (1 - c) + q_ * c
        y_ = q_ * (1 - c) + p_ * c
        return (x_ * side + y_) * 2 + c_

    ppos = [lax.rem(p + j, side) for j in range(side)]
    qpos = [lax.rem(q + j, side) for j in range(side)]
    pdev = [dev(v, q, c) for v in ppos]
    qdev = [dev(p, v, c) for v in qpos]
    partner = dev(p, q, 1 - c)

    def pick(vals, k, way):
        u, v = (vals[1], vals[side - 1]) if way > 0 else (vals[side - 1], vals[1])
        return v if k % 2 else u

    def remote(kind, slot, i, k, src, dst, to):
        return pltpu.make_async_remote_copy(
            src_ref=src, dst_ref=dst, send_sem=ss.at[KINDS.index(kind), slot], recv_sem=rs.at[i, k],
            device_id={"dp": to}, device_id_type=pl.DeviceIdType.MESH)

    flying = {kind: [] for kind in KINDS}
    count = {kind: 0 for kind in KINDS}

    def land(kind):
        slot = (count[kind] - len(flying[kind])) % SLOTS
        size = flying[kind].pop(0)
        remote(kind, slot, 0, 0, size, size, partner).wait_send()

    def send(kind, k, size, *copies):
        if len(flying[kind]) == SLOTS:
            land(kind)
        for i, src, dst, to in copies:
            remote(kind, count[kind] % SLOTS, i, k, src, dst, to).start()
        flying[kind].append(size)
        count[kind] += 1

    def recv(i, k, size):
        remote("A", 0, i, k, size, size, partner).wait_recv()

    def quarter(i):
        return pl.ds(pl.multiple_of(i * (rows // side), rows // side), rows // side)

    quarters = [None] + [rb.at[0, pl.ds(0, m)] for m in (1, 2, 3)]
    half, pieces = xr.at[0], ub.at[0]

    def send_a(k):
        send("A", k, half, (0, xs.at[k], xr.at[k], partner))

    def wait_b(k):
        recv(0, k, half)

    def work_b(k):
        def part(i):
            return acc[k % RING, quarter(i), :] + xr[k, quarter(i), :].astype(F32)

        if k in DIRECT:
            for j in (2, 1, 3):
                sb[k, j - 1] = part(ppos[j]).astype(BF)
        else:
            sb[k, 0] = part(ppos[2]).astype(BF)
            sb[k, 1] = part(pick(ppos, k, -1)).astype(BF)
            cs[k, 0] = part(pick(ppos, k, 1))
        cs[k, 1] = part(p)

    def send_b(k):
        if k in DIRECT:
            send("B", k, quarters[3], *((2, sb.at[k, j - 1], rb.at[k, j - 1], pdev[j]) for j in (2, 1, 3)))
        else:
            send("B", k, quarters[2], (1, sb.at[k, 0], rb.at[k, 0], pick(pdev, k, 1)),
                 (2, sb.at[k, 1], rb.at[k, 1], pick(pdev, k, -1)))

    def wait_c(k):
        recv(1, k, quarters[1])

    def work_c(k):
        sb[k, 2] = (cs[k, 0] + rb[k, 0].astype(F32)).astype(BF)

    def send_c(k):
        send("C", k, quarters[1], (2, sb.at[k, 2], rb.at[k, 2], pick(pdev, k, 1)))

    def wait_d(k):
        recv(2, k, quarters[3 if k in DIRECT else 2])

    def work_d(k):
        tot = cs[k, 1] + rb[k, 1].astype(F32) + rb[k, 2].astype(F32)
        if k in DIRECT:
            tot = tot + rb[k, 0].astype(F32)
        if k in FUSED:
            fr[FUSED.index(k), q] = tot.astype(BF)
            return
        ps[k] = tot.reshape(ps.shape[1:])
        for j in (2, 1, 3):
            tb[k, j - 1] = ps[k, qpos[j]].astype(BF)

    def send_d(k):
        if k in FUSED:
            mine = fr.at[FUSED.index(k), q]
            send("D", k, quarters[3], *((4, mine, mine, qdev[j]) for j in (2, 1, 3)))
        else:
            send("D", k, pieces, *((3, tb.at[k, j - 1], ub.at[k, j - 1], qdev[j]) for j in (2, 1, 3)))

    def wait_f(k):
        recv(3, k, pieces)

    def work_f(k):
        tot = ps[k, q] + ub[k, 0].astype(F32) + ub[k, 1].astype(F32) + ub[k, 2].astype(F32)
        o_ref[k, c, p, q] = tot.astype(BF)

    def send_f(k):
        mine = o_ref.at[k, c, p, q]
        send("F", k, pieces, *((4, mine, mine, qdev[j]) for j in (2, 1, 3)))

    def wait_h(k):
        recv(4, k, quarters[3] if k in FUSED else pieces)

    def work_h(k):
        if k in FUSED:
            f = FUSED.index(k)
            tot = fr[f, 0].astype(F32)
            for j in range(1, side):
                tot = tot + fr[f, j].astype(F32)
            o_ref[k, c, p] = tot.reshape(o_ref.shape[3:]).astype(BF)

    def across(k, j, to, i=7):
        quad = o_ref.at[k, c, ppos[j] if isinstance(j, int) else j]
        return i, quad, quad, to

    def send_h(k):
        if k in SPREAD:
            send("H", k, quarters[3], *(across(k, 0, pdev[j], 6) for j in (2, 1, 3)))
        else:
            send("H", k, quarters[2], *(across(k, 0, pdev[j], 5) for j in (1, side - 1)))
        send("P", k, quarters[1], across(k, 0, partner))

    def stage_i(k):
        recv(5, k, quarters[2])
        send("I", k, quarters[1], across(k, pick(ppos, k, -1), pick(pdev, k, 1), 6))
        send("P", k, quarters[2], across(k, 1, partner), across(k, side - 1, partner))

    def stage_j(k):
        if k in SPREAD:
            recv(6, k, quarters[3])
            send("P", k, quarters[3], *(across(k, j, partner) for j in (1, 2, 3)))
        else:
            recv(6, k, quarters[1])
            send("P", k, quarters[1], across(k, 2, partner))

    def stage_l(k):
        recv(7, k, half)

    waits = dict(B=wait_b, C=wait_c, D=wait_d, F=wait_f, H=wait_h)
    works = dict(B=work_b, C=work_c, D=work_d, F=work_f, H=work_h)
    sends = dict(A=send_a, B=send_b, C=send_c, D=send_d, F=send_f, H=send_h)
    whole = dict(I=stage_i, J=stage_j, L=stage_l)

    def stage(name, k):
        if name in whole:
            whole[name](k)
        else:
            waits[name](k)
            works[name](k)
            sends[name](k)

    barrier = pltpu.get_barrier_semaphore()
    for to in [partner] + pdev[1:] + qdev[1:]:
        pl.semaphore_signal(barrier, inc=1, device_id={"dp": to}, device_id_type=pl.DeviceIdType.MESH)

    def gcopies(k):
        def half(i):
            col = pl.multiple_of((2 * (k % per) + lax.rem(c + i, 2)) * W, W)
            return pltpu.make_async_copy(
                g_ref.at[0, k // per, :, pl.ds(col, W)], gb.at[k % 2, :, pl.ds(i * W, W)], gsem.at[i, k % 2])
        return half(0), half(1)

    def acopy(m, b):
        return pltpu.make_async_copy(a_ref.at[0, m, pl.ds(b * TB, TB), :], ast.at[b], asem.at[b])

    def turn(m, b):
        at[m, :, pl.ds(b * TB if isinstance(b, int) else pl.multiple_of(b * TB, TB), TB)] = ast[b].T

    nb = tokens // TB
    for b in range(nb):
        acopy(0, b).start()
    for copy in gcopies(0):
        copy.start()
    with jax.named_scope("head"):
        def first(b, _):
            acopy(0, b).wait()
            turn(0, b)
            acopy(1, b).start()
            return 0
        lax.fori_loop(0, nb, first, 0)
    pl.semaphore_wait(barrier, 1 + 2 * (side - 1))

    done = 0
    for t in range(K):
        with jax.named_scope("top"):
            for copy in gcopies(t + 1) if t + 1 < K else ():
                copy.start()
            beside = []
            for item in STEPS[t]:
                name, k = item[0].upper(), int(item[1:])
                if item[0] == name:
                    stage(name, k)
                else:
                    waits[name](k)
                    beside.append((name, k))
            turns = range(done, min(done + 2, nb))
            done += len(turns)
            for b in turns:
                acopy(1, b).wait()
            for copy in gcopies(t):
                copy.wait()
        with jax.named_scope("dot"):
            @pl.when(me >= 0)
            def _():
                for b in turns:
                    turn(1, b)
                for name, k in beside:
                    works[name](k)
                res = jnp.dot(at[t // per], gb[t % 2], preferred_element_type=F32)
                acc[t % RING] = res[:, :W]
                xs[t] = res[:, W:].astype(BF)
        with jax.named_scope("end"):
            send_a(t)
            for name, k in beside:
                sends[name](k)
    for item in DRAIN:
        with jax.named_scope(item):
            stage(item[0], int(item[1:]))
    for kind in KINDS:
        while flying[kind]:
            land(kind)


def write(o_ref, out_ref, sem):
    w = o_ref.shape[-1]
    per = out_ref.shape[2] // w
    blocks = out_ref.shape[0] * per

    def copy(k):
        return pltpu.make_async_copy(
            o_ref.at[k], out_ref.at[k // per, :, pl.ds(k % per * w, w)], sem.at[k])

    for k in range(blocks):
        copy(k).start()
    for k in range(blocks):
        copy(k).wait()


def solution(mesh):
    n = mesh.shape["dp"]
    side = math.isqrt(n // 2)

    def step(a, g):
        _, mats, tokens, rows = a.shape
        cols = g.shape[-1]
        K = mats * cols // (2 * W)
        quarter, piece = rows // side, rows // side // side
        o = pl.pallas_call(
            functools.partial(kernel, n, mats, tokens, rows, cols),
            out_shape=pltpu.VMEM((K, 2, side, side, piece, W), BF),
            in_specs=[pl.BlockSpec(memory_space=pl.ANY)] * 2,
            out_specs=pl.BlockSpec(memory_space=pltpu.VMEM),
            scratch_shapes=[
                pltpu.VMEM((mats, rows, tokens), BF),
                pltpu.VMEM((tokens // TB, TB, rows), BF),
                pltpu.VMEM((2, tokens, 2 * W), BF),
                pltpu.VMEM((RING, rows, W), F32),
                pltpu.VMEM((K, rows, W), BF),
                pltpu.VMEM((K, rows, W), BF),
                pltpu.VMEM((K, 2, quarter, W), F32),
                pltpu.VMEM((K, 3, quarter, W), BF),
                pltpu.VMEM((K, 3, quarter, W), BF),
                pltpu.VMEM((K, side, piece, W), F32),
                pltpu.VMEM((K, 3, piece, W), BF),
                pltpu.VMEM((K, 3, piece, W), BF),
                pltpu.VMEM((max(len(FUSED), 1), side, quarter, W), BF),
                pltpu.SemaphoreType.DMA((tokens // TB,)),
                pltpu.SemaphoreType.DMA((2, 2)),
                pltpu.SemaphoreType.DMA((len(KINDS), SLOTS)),
                pltpu.SemaphoreType.DMA((8, K)),
            ],
            name="sums",
            compiler_params=pltpu.CompilerParams(
                collective_id=0, has_side_effects=True, vmem_limit_bytes=55 * 2**20),
        )(a, g)
        o = o.reshape(K * 2, rows, W)
        return pl.pallas_call(
            write,
            out_shape=jax.ShapeDtypeStruct((mats, rows, cols), BF),
            in_specs=[pl.BlockSpec(memory_space=pltpu.VMEM)],
            out_specs=pl.BlockSpec(memory_space=pl.ANY),
            scratch_shapes=[pltpu.SemaphoreType.DMA((K * 2,))],
            name="write",
            compiler_params=pltpu.CompilerParams(vmem_limit_bytes=8 * 2**20),
        )(pltpu.with_memory_space_constraint(o, pltpu.VMEM))

    return jax.shard_map(
        step, mesh=mesh, in_specs=(P(("rep", "dp")), P(("rep", "dp"))), out_specs=P("rep"), check_vma=False)
```

```python
import functools
import math

import jax
import jax.numpy as jnp
from jax import lax
from jax.experimental import pallas as pl
from jax.experimental.pallas import tpu as pltpu
from jax.sharding import PartitionSpec as P

BF, F32 = jnp.bfloat16, jnp.float32
W = 128
TB = 512
RING = 4
KINDS = "ABDFHP"
DIRECT, SPREAD, NEAR = (0, 1, 2, 3, 4, 5, 6, 7, 8, 15, 16, 17,), (16, 17,), ()
STEPS = (
    (),
    (),
    ("B0",),
    ("b1",),
    ("d0", "b2",),
    ("B3",),
    ("d1", "B4",),
    ("D2", "B5", "f0",),
    ("D3", "B6", "D4",),
    ("F1", "B7", "F2", "D5",),
    ("H0", "d6", "F3", "B8",),
    ("D7", "F4", "B9", "H1", "H2",),
    ("B10", "F5", "H3", "D8",),
    ("H4", "F7", "I0", "C9", "B11", "F6",),
    ("I1", "I2", "H5", "C10", "B12", "I3",),
    ("B13", "D9", "I4", "H7", "C11",),
    ("B14", "f8", "H6", "C12", "C13", "D10", "B15",),
    ("D11", "I5", "C14", "d13", "F9", "J3", "B16", "D12", "I6", "I7",),
)
DRAIN = (
    "F10", "D15", "D14", "B17", "D16", "J0", "F11", "H8", "H9", "F14", "F13", "F15", "D17", "J1", "F12", "H10", "H11",
    "F16", "I9", "J2", "I8", "H13", "F17", "H15", "H14", "I11", "H12", "H16", "I10", "H17", "J4", "I13", "I14", "I15",
    "J8", "I12", "J5", "J6", "J16", "J10", "J11", "J7", "J9", "J14", "J13", "J17", "J12", "J15",
)


def kernel(n, mats, tokens, rows, cols, a_ref, g_ref, o_ref,
           at, ast, t0, t1, gb, acc, first, xs, xr, cs, sb, rb, ps, tb, ub,
           asem, gsem, hsem, ss, rs, rl):
    side = math.isqrt(n // 2)
    per = cols // (2 * W)
    K = mats * per
    me = lax.axis_index("dp")
    c = lax.rem(me, 2)
    y = lax.rem(me // 2, side)
    x = me // (2 * side)
    p = x * (1 - c) + y * c
    q = y * (1 - c) + x * c

    def dev(p_, q_, c_):
        x_ = p_ * (1 - c) + q_ * c
        y_ = q_ * (1 - c) + p_ * c
        return (x_ * side + y_) * 2 + c_

    ppos = [lax.rem(p + j, side) for j in range(side)]
    qpos = [lax.rem(q + j, side) for j in range(side)]
    pdev = [dev(v, q, c) for v in ppos]
    qdev = [dev(p, v, c) for v in qpos]
    partner = dev(p, q, 1 - c)

    def pick(vals, k, way):
        u, v = (vals[1], vals[side - 1]) if way > 0 else (vals[side - 1], vals[1])
        return v if k % 2 else u

    def remote(kind, i, k, src, dst, to):
        return pltpu.make_async_remote_copy(
            src_ref=src, dst_ref=dst, send_sem=ss.at[KINDS.index(kind)], recv_sem=rl if i == 7 else rs.at[i, k],
            device_id={"dp": to}, device_id_type=pl.DeviceIdType.MESH)

    def send(kind, k, *copies):
        for i, src, dst, to in copies:
            remote(kind, i, k, src, dst, to).start()

    def recv(i, k, size):
        remote("A", i, k, size, size, partner).wait_recv()

    lanes = pl.ds(pl.multiple_of(c * W, W), W)

    def quarter(i):
        return pl.ds(pl.multiple_of(i * (rows // side), rows // side), rows // side)

    quarters = [None] + [rb.at[0, pl.ds(0, m)] for m in (1, 2, 3)]
    pieces = [None] + [ub.at[0, pl.ds(0, m)] for m in (1, 2, 3)]
    half = xr.at[0]

    def send_a(k):
        send("A", k, (0, xs.at[k], xr.at[k], partner))

    def wait_b(k):
        recv(0, k, half)

    def work_b(k):
        def part(i):
            return acc[k % RING, quarter(i), :] + xr[k, quarter(i), :].astype(F32)

        if k in DIRECT:
            for j in (2, 1, 3):
                sb[k, j - 1] = part(ppos[j]).astype(BF)
        else:
            sb[k, 0] = part(ppos[2]).astype(BF)
            sb[k, 1] = part(pick(ppos, k, -1)).astype(BF)
            cs[k, 0] = part(pick(ppos, k, 1))
        cs[k, 1] = part(p)

    def send_b(k):
        if k in DIRECT:
            send("B", k, *((2, sb.at[k, j - 1], rb.at[k, j - 1], pdev[j]) for j in (2, 1, 3)))
        else:
            send("B", k, (1, sb.at[k, 0], rb.at[k, 0], pick(pdev, k, 1)),
                 (2, sb.at[k, 1], rb.at[k, 1], pick(pdev, k, -1)))

    def wait_c(k):
        recv(1, k, quarters[1])

    def work_c(k):
        sb[k, 2] = (cs[k, 0] + rb[k, 0].astype(F32)).astype(BF)

    def send_c(k):
        send("B", k, (2, sb.at[k, 2], rb.at[k, 2], pick(pdev, k, 1)))

    def wait_d(k):
        recv(2, k, quarters[3 if k in DIRECT else 2])

    def work_d(k):
        tot = cs[k, 1] + rb[k, 1].astype(F32) + rb[k, 2].astype(F32)
        if k in DIRECT:
            tot = tot + rb[k, 0].astype(F32)
        ps[k] = tot.reshape(ps.shape[1:])
        if k in NEAR:
            tb[k, 1] = ps[k, qpos[2]].astype(BF)
            tb[k, 0] = ps[k, pick(qpos, k, -1)].astype(BF)
        else:
            for j in (2, 1, 3):
                tb[k, j - 1] = ps[k, qpos[j]].astype(BF)

    def send_d(k):
        if k in NEAR:
            send("D", k, (8, tb.at[k, 1], ub.at[k, 1], pick(qdev, k, 1)),
                 (3, tb.at[k, 0], ub.at[k, 0], pick(qdev, k, -1)))
        else:
            send("D", k, *((3, tb.at[k, j - 1], ub.at[k, j - 1], qdev[j]) for j in (2, 1, 3)))

    def wait_e(k):
        recv(8, k, pieces[1])

    def work_e(k):
        tb[k, 2] = (ps[k, pick(qpos, k, 1)] + ub[k, 1].astype(F32)).astype(BF)

    def send_e(k):
        send("D", k, (3, tb.at[k, 2], ub.at[k, 2], pick(qdev, k, 1)))

    def wait_f(k):
        recv(3, k, pieces[2 if k in NEAR else 3])

    def work_f(k):
        tot = ps[k, q] + ub[k, 0].astype(F32) + ub[k, 2].astype(F32)
        if k not in NEAR:
            tot = tot + ub[k, 1].astype(F32)
        o_ref[k, p, q, :, lanes] = tot.astype(BF)

    def send_f(k):
        mine = o_ref.at[k, p, q, :, lanes]
        if k in NEAR:
            send("F", k, (9, mine, mine, pick(qdev, k, 1)), (4, mine, mine, pick(qdev, k, -1)))
        else:
            send("F", k, *((4, mine, mine, qdev[j]) for j in (2, 1, 3)))

    def stage_g(k):
        recv(9, k, pieces[1])
        piece = o_ref.at[k, p, pick(qpos, k, -1), :, lanes]
        send("F", k, (4, piece, piece, pick(qdev, k, 1)))

    def wait_h(k):
        recv(4, k, pieces[2 if k in NEAR else 3])

    def work_h(k):
        pass

    def across(k, j, to, i=7):
        quad = o_ref.at[k, ppos[j] if isinstance(j, int) else j, :, :, lanes]
        return i, quad, quad, to

    def send_h(k):
        if k in SPREAD:
            send("H", k, *(across(k, 0, pdev[j], 6) for j in (2, 1, 3)))
        else:
            send("H", k, *(across(k, 0, pdev[j], 5) for j in (1, side - 1)))
        send("P", k, across(k, 0, partner))

    def stage_i(k):
        recv(5, k, quarters[2])
        send("H", k, across(k, pick(ppos, k, -1), pick(pdev, k, 1), 6))
        send("P", k, across(k, 1, partner), across(k, side - 1, partner))

    def stage_j(k):
        if k in SPREAD:
            recv(6, k, quarters[3])
            send("P", k, *(across(k, j, partner) for j in (1, 2, 3)))
        else:
            recv(6, k, quarters[1])
            send("P", k, across(k, 2, partner))

    waits = dict(B=wait_b, C=wait_c, D=wait_d, E=wait_e, F=wait_f, H=wait_h)
    works = dict(B=work_b, C=work_c, D=work_d, E=work_e, F=work_f, H=work_h)
    sends = dict(A=send_a, B=send_b, C=send_c, D=send_d, E=send_e, F=send_f, H=send_h)
    whole = dict(G=stage_g, I=stage_i, J=stage_j)

    def stage(name, k):
        if name in whole:
            whole[name](k)
        else:
            waits[name](k)
            works[name](k)
            sends[name](k)

    barrier = pltpu.get_barrier_semaphore()
    for to in [partner] + pdev[1:] + qdev[1:]:
        pl.semaphore_signal(barrier, inc=1, device_id={"dp": to}, device_id_type=pl.DeviceIdType.MESH)

    def gcopies(k):
        def half(i):
            col = pl.multiple_of((2 * (k % per) + lax.rem(c + i, 2)) * W, W)
            return pltpu.make_async_copy(
                g_ref.at[0, k // per, :, pl.ds(col, W)], gb.at[k % 2, :, pl.ds(i * W, W)], gsem.at[i, k % 2])
        return half(0), half(1)

    def acopy(m, b):
        return pltpu.make_async_copy(a_ref.at[0, m, pl.ds(b * TB, TB), :], ast.at[b], asem.at[b])

    nb = tokens // TB
    blocks = (t0, t1)

    def hcopies(b):
        return [pltpu.make_async_copy(
            g_ref.at[0, 0, pl.ds(b * TB, TB), pl.ds(pl.multiple_of(lax.rem(c + i, 2) * W, W), W)],
            gb.at[0, pl.ds(b * TB, TB), pl.ds(i * W, W)], hsem.at[i, b]) for i in range(2)]

    for b in range(nb):
        for copy in [acopy(0, b)] + hcopies(b):
            copy.start()
    first[...] = jnp.zeros_like(first)
    with jax.named_scope("head"):
        acopy(0, 0).wait()
        t0[...] = ast[0].T
        at[0, :, 0:TB] = t0[...]

        def head(i, _):
            for s in range(2):
                b = 2 * i + s
                nxt = lax.min(b + 1, nb - 1)

                @pl.when(b + 1 < nb)
                def _():
                    acopy(0, nxt).wait()

                for copy in hcopies(b):
                    copy.wait()

                @pl.when(me >= 0)
                def _():
                    t = ast[nxt].T
                    blocks[1 - s][...] = t
                    at[0, :, pl.ds(pl.multiple_of(nxt * TB, TB), TB)] = t
                    first[...] += jnp.dot(
                        blocks[s][...], gb[0, pl.ds(pl.multiple_of(b * TB, TB), TB)], preferred_element_type=F32)

            @pl.when(i == 1)
            def _():
                for copy in gcopies(1):
                    copy.start()
            return 0

        lax.fori_loop(0, nb // 2, head, 0)
    for copy in gcopies(2):
        copy.start()
    xs[0] = first[:, W:].astype(BF)
    pl.semaphore_wait(barrier, 1 + 2 * (side - 1))
    send_a(0)
    acc[0] = first[:, :W]

    done = 0
    for t in range(1, K):
        with jax.named_scope("top"):
            for copy in gcopies(t + 1) if 1 < t < K - 1 else ():
                copy.start()
            for b in range(2 * t - 2, min(2 * t, nb)):
                acopy(1, b).start()
            beside = []
            for item in STEPS[t]:
                name, k = item[0].upper(), int(item[1:])
                if item[0] == name:
                    stage(name, k)
                else:
                    waits[name](k)
                    beside.append((name, k))
            turns = range(done, min(done + 2, nb)) if t > 2 else ()
            done += len(turns)
            for b in turns:
                acopy(1, b).wait()
            for copy in gcopies(t):
                copy.wait()
        with jax.named_scope("dot"):
            @pl.when(me >= 0)
            def _():
                for b in turns:
                    at[1, :, b * TB:(b + 1) * TB] = ast[b].T
                for name, k in beside:
                    works[name](k)
                res = jnp.dot(at[t // per], gb[t % 2], preferred_element_type=F32)
                acc[t % RING] = res[:, :W]
                xs[t] = res[:, W:].astype(BF)
        with jax.named_scope("end"):
            send_a(t)
            for name, k in beside:
                sends[name](k)
    for item in DRAIN:
        with jax.named_scope(item):
            stage(item[0], int(item[1:]))
    recv(7, 0, xr)
    for kind, size in zip(KINDS, (xs, sb, tb, tb, sb, xs)):
        remote(kind, 0, 0, size, size, partner).wait_send()


def write(o_ref, out_ref, sem):
    w = o_ref.shape[-1]
    per = out_ref.shape[2] // w
    blocks = out_ref.shape[0] * per

    def copy(k):
        return pltpu.make_async_copy(
            o_ref.at[k], out_ref.at[k // per, :, pl.ds(k % per * w, w)], sem.at[k])

    for k in range(blocks):
        copy(k).start()
    for k in range(blocks):
        copy(k).wait()


def solution(mesh):
    n = mesh.shape["dp"]
    side = math.isqrt(n // 2)

    def step(a, g):
        _, mats, tokens, rows = a.shape
        cols = g.shape[-1]
        K = mats * cols // (2 * W)
        quarter, piece = rows // side, rows // side // side
        o = pl.pallas_call(
            functools.partial(kernel, n, mats, tokens, rows, cols),
            out_shape=pltpu.VMEM((K, side, side, piece, 2 * W), BF),
            in_specs=[pl.BlockSpec(memory_space=pl.ANY)] * 2,
            out_specs=pl.BlockSpec(memory_space=pltpu.VMEM),
            scratch_shapes=[
                pltpu.VMEM((mats, rows, tokens), BF),
                pltpu.VMEM((tokens // TB, TB, rows), BF),
                pltpu.VMEM((rows, TB), BF),
                pltpu.VMEM((rows, TB), BF),
                pltpu.VMEM((2, tokens, 2 * W), BF),
                pltpu.VMEM((RING, rows, W), F32),
                pltpu.VMEM((rows, 2 * W), F32),
                pltpu.VMEM((K, rows, W), BF),
                pltpu.VMEM((K, rows, W), BF),
                pltpu.VMEM((K, 2, quarter, W), F32),
                pltpu.VMEM((K, 3, quarter, W), BF),
                pltpu.VMEM((K, 3, quarter, W), BF),
                pltpu.VMEM((K, side, piece, W), F32),
                pltpu.VMEM((K, 3, piece, W), BF),
                pltpu.VMEM((K, 3, piece, W), BF),
                pltpu.SemaphoreType.DMA((tokens // TB,)),
                pltpu.SemaphoreType.DMA((2, 2)),
                pltpu.SemaphoreType.DMA((2, tokens // TB)),
                pltpu.SemaphoreType.DMA((len(KINDS),)),
                pltpu.SemaphoreType.DMA((10 if NEAR else 7, K)),
                pltpu.SemaphoreType.DMA,
            ],
            name="sums",
            compiler_params=pltpu.CompilerParams(
                collective_id=0, has_side_effects=True, vmem_limit_bytes=55 * 2**20),
        )(a, g)
        o = o.reshape(K, rows, 2 * W)
        return pl.pallas_call(
            write,
            out_shape=jax.ShapeDtypeStruct((mats, rows, cols), BF),
            in_specs=[pl.BlockSpec(memory_space=pltpu.VMEM)],
            out_specs=pl.BlockSpec(memory_space=pl.ANY),
            scratch_shapes=[pltpu.SemaphoreType.DMA((K,))],
            name="write",
            compiler_params=pltpu.CompilerParams(vmem_limit_bytes=8 * 2**20),
        )(pltpu.with_memory_space_constraint(o, pltpu.VMEM))

    return jax.shard_map(
        step, mesh=mesh, in_specs=(P(("rep", "dp")), P(("rep", "dp"))), out_specs=P("rep"), check_vma=False)
```

```python
import functools
import math

import jax
import jax.numpy as jnp
from jax import lax
from jax.experimental import pallas as pl
from jax.experimental.pallas import tpu as pltpu
from jax.sharding import PartitionSpec as P

BF, F32 = jnp.bfloat16, jnp.float32
W = 128
TB = 512
RING = 4
KINDS = "ABDFHP"
DIRECT, SPREAD, NEAR = (0, 1, 2, 3, 4, 5, 6, 7, 8, 15, 16, 17,), (16, 17,), ()
STEPS = (
    (),
    (),
    ("b0",),
    ("b1",),
    ("b2",),
    ("d0", "B3",),
    ("D1", "B4",),
    ("D2", "B5", "D3",),
    ("F1", "F0", "B6", "D4",),
    ("F2", "D5", "B7", "F3", "H1",),
    ("B8", "f4", "d6", "H0",),
    ("H2", "D7", "b9", "f5", "H3",),
    ("B10", "D8", "I0", "I1",),
    ("B11", "I2", "F7", "F6", "H4", "I3",),
    ("C10", "C9", "F8", "B12", "H5",),
    ("B13", "C11", "H7", "I4", "H6", "J2",),
    ("D9", "B14", "C12", "H8", "D10", "C13",),
    ("D11", "B15", "I5", "J0", "J3", "F9", "I7", "C14", "D13", "d12", "F10", "B16", "I6",),
)
DRAIN = (
    "D15", "D14", "F11", "J1", "J4", "B17", "F13", "H9", "D16", "H10", "F15", "J5", "F14", "F12", "H11", "D17", "F16",
    "H13", "H15", "H14", "H12", "F17", "H16", "I9", "I8", "I14", "I11", "I10", "J6", "I15", "I13", "I12", "H17", "J15",
    "J14", "J13", "J11", "J7", "J8", "J16", "J12", "J9", "J10", "J17",
)


def kernel(n, mats, tokens, rows, cols, a_ref, g_ref, o_ref,
           at, ast, t0, t1, gb, acc, first, xs, xr, cs, sb, rb, ps, tb, ub,
           asem, gsem, hsem, ss, rs, rl):
    side = math.isqrt(n // 2)
    per = cols // (2 * W)
    K = mats * per
    me = lax.axis_index("dp")
    c = lax.rem(me, 2)
    y = lax.rem(me // 2, side)
    x = me // (2 * side)
    p = x * (1 - c) + y * c
    q = y * (1 - c) + x * c

    def dev(p_, q_, c_):
        x_ = p_ * (1 - c) + q_ * c
        y_ = q_ * (1 - c) + p_ * c
        return (x_ * side + y_) * 2 + c_

    ppos = [lax.rem(p + j, side) for j in range(side)]
    qpos = [lax.rem(q + j, side) for j in range(side)]
    pdev = [dev(v, q, c) for v in ppos]
    qdev = [dev(p, v, c) for v in qpos]
    partner = dev(p, q, 1 - c)

    def pick(vals, k, way):
        u, v = (vals[1], vals[side - 1]) if way > 0 else (vals[side - 1], vals[1])
        return v if k % 2 else u

    def remote(kind, i, k, src, dst, to):
        return pltpu.make_async_remote_copy(
            src_ref=src, dst_ref=dst, send_sem=ss.at[KINDS.index(kind)], recv_sem=rl if i == 7 else rs.at[i, k],
            device_id={"dp": to}, device_id_type=pl.DeviceIdType.MESH)

    def send(kind, k, *copies):
        for i, src, dst, to in copies:
            remote(kind, i, k, src, dst, to).start()

    def recv(i, k, size):
        remote("A", i, k, size, size, partner).wait_recv()

    lanes = pl.ds(pl.multiple_of(c * W, W), W)

    def quarter(i):
        return pl.ds(pl.multiple_of(i * (rows // side), rows // side), rows // side)

    quarters = [None] + [rb.at[0, pl.ds(0, m)] for m in (1, 2, 3)]
    pieces = [None] + [ub.at[0, pl.ds(0, m)] for m in (1, 2, 3)]
    half = xr.at[0]

    def send_a(k):
        send("A", k, (0, xs.at[k], xr.at[k], partner))

    def wait_b(k):
        recv(0, k, half)

    def work_b(k):
        def part(i):
            return acc[k % RING, quarter(i), :] + xr[k, quarter(i), :].astype(F32)

        if k in DIRECT:
            for j in (2, 1, 3):
                sb[k, j - 1] = part(ppos[j]).astype(BF)
        else:
            sb[k, 0] = part(ppos[2]).astype(BF)
            sb[k, 1] = part(pick(ppos, k, -1)).astype(BF)
            cs[k, 0] = part(pick(ppos, k, 1))
        cs[k, 1] = part(p)

    def send_b(k):
        if k in DIRECT:
            send("B", k, *((2, sb.at[k, j - 1], rb.at[k, j - 1], pdev[j]) for j in (2, 1, 3)))
        else:
            send("B", k, (1, sb.at[k, 0], rb.at[k, 0], pick(pdev, k, 1)),
                 (2, sb.at[k, 1], rb.at[k, 1], pick(pdev, k, -1)))

    def wait_c(k):
        recv(1, k, quarters[1])

    def work_c(k):
        sb[k, 2] = (cs[k, 0] + rb[k, 0].astype(F32)).astype(BF)

    def send_c(k):
        send("B", k, (2, sb.at[k, 2], rb.at[k, 2], pick(pdev, k, 1)))

    def wait_d(k):
        recv(2, k, quarters[3 if k in DIRECT else 2])

    def work_d(k):
        tot = cs[k, 1] + rb[k, 1].astype(F32) + rb[k, 2].astype(F32)
        if k in DIRECT:
            tot = tot + rb[k, 0].astype(F32)
        ps[k] = tot.reshape(ps.shape[1:])
        if k in NEAR:
            tb[k, 1] = ps[k, qpos[2]].astype(BF)
            tb[k, 0] = ps[k, pick(qpos, k, -1)].astype(BF)
        else:
            for j in (2, 1, 3):
                tb[k, j - 1] = ps[k, qpos[j]].astype(BF)

    def send_d(k):
        if k in NEAR:
            send("D", k, (8, tb.at[k, 1], ub.at[k, 1], pick(qdev, k, 1)),
                 (3, tb.at[k, 0], ub.at[k, 0], pick(qdev, k, -1)))
        else:
            send("D", k, *((3, tb.at[k, j - 1], ub.at[k, j - 1], qdev[j]) for j in (2, 1, 3)))

    def wait_e(k):
        recv(8, k, pieces[1])

    def work_e(k):
        tb[k, 2] = (ps[k, pick(qpos, k, 1)] + ub[k, 1].astype(F32)).astype(BF)

    def send_e(k):
        send("D", k, (3, tb.at[k, 2], ub.at[k, 2], pick(qdev, k, 1)))

    def wait_f(k):
        recv(3, k, pieces[2 if k in NEAR else 3])

    def work_f(k):
        tot = ps[k, q] + ub[k, 0].astype(F32) + ub[k, 2].astype(F32)
        if k not in NEAR:
            tot = tot + ub[k, 1].astype(F32)
        o_ref[k, p, q, :, lanes] = tot.astype(BF)

    def send_f(k):
        mine = o_ref.at[k, p, q, :, lanes]
        if k in NEAR:
            send("F", k, (9, mine, mine, pick(qdev, k, 1)), (4, mine, mine, pick(qdev, k, -1)))
        else:
            send("F", k, *((4, mine, mine, qdev[j]) for j in (2, 1, 3)))

    def stage_g(k):
        recv(9, k, pieces[1])
        piece = o_ref.at[k, p, pick(qpos, k, -1), :, lanes]
        send("F", k, (4, piece, piece, pick(qdev, k, 1)))

    def wait_h(k):
        recv(4, k, pieces[2 if k in NEAR else 3])

    def work_h(k):
        pass

    def across(k, j, to, i=7):
        quad = o_ref.at[k, ppos[j] if isinstance(j, int) else j, :, :, lanes]
        return i, quad, quad, to

    def send_h(k):
        if k in SPREAD:
            send("H", k, *(across(k, 0, pdev[j], 6) for j in (2, 1, 3)))
        else:
            send("H", k, *(across(k, 0, pdev[j], 5) for j in (1, side - 1)))
        send("P", k, across(k, 0, partner))

    def stage_i(k):
        recv(5, k, quarters[2])
        send("H", k, across(k, pick(ppos, k, -1), pick(pdev, k, 1), 6))
        send("P", k, across(k, 1, partner), across(k, side - 1, partner))

    def stage_j(k):
        if k in SPREAD:
            recv(6, k, quarters[3])
            send("P", k, *(across(k, j, partner) for j in (1, 2, 3)))
        else:
            recv(6, k, quarters[1])
            send("P", k, across(k, 2, partner))

    waits = dict(B=wait_b, C=wait_c, D=wait_d, E=wait_e, F=wait_f, H=wait_h)
    works = dict(B=work_b, C=work_c, D=work_d, E=work_e, F=work_f, H=work_h)
    sends = dict(A=send_a, B=send_b, C=send_c, D=send_d, E=send_e, F=send_f, H=send_h)
    whole = dict(G=stage_g, I=stage_i, J=stage_j)

    def stage(name, k):
        if name in whole:
            whole[name](k)
        else:
            waits[name](k)
            works[name](k)
            sends[name](k)

    barrier = pltpu.get_barrier_semaphore()
    for to in [partner] + pdev[1:] + qdev[1:]:
        pl.semaphore_signal(barrier, inc=1, device_id={"dp": to}, device_id_type=pl.DeviceIdType.MESH)

    def gcopies(k):
        def half(i):
            col = pl.multiple_of((2 * (k % per) + lax.rem(c + i, 2)) * W, W)
            return pltpu.make_async_copy(
                g_ref.at[0, k // per, :, pl.ds(col, W)], gb.at[k % 2, :, pl.ds(i * W, W)], gsem.at[i, k % 2])
        return half(0), half(1)

    def acopy(m, b):
        return pltpu.make_async_copy(a_ref.at[0, m, pl.ds(b * TB, TB), :], ast.at[b], asem.at[b])

    nb = tokens // TB
    blocks = (t0, t1)

    def hcopies(b):
        return [pltpu.make_async_copy(
            g_ref.at[0, 0, pl.ds(b * TB, TB), pl.ds(pl.multiple_of(lax.rem(c + i, 2) * W, W), W)],
            gb.at[0, pl.ds(b * TB, TB), pl.ds(i * W, W)], hsem.at[i, b]) for i in range(2)]

    for b in range(nb):
        for copy in [acopy(0, b)] + hcopies(b):
            copy.start()
    first[...] = jnp.zeros_like(first)
    with jax.named_scope("head"):
        acopy(0, 0).wait()
        t0[...] = ast[0].T
        at[0, :, 0:TB] = t0[...]

        def head(i, _):
            for s in range(2):
                b = 2 * i + s
                nxt = lax.min(b + 1, nb - 1)

                @pl.when(b + 1 < nb)
                def _():
                    acopy(0, nxt).wait()

                for copy in hcopies(b):
                    copy.wait()

                @pl.when(me >= 0)
                def _():
                    t = ast[nxt].T
                    blocks[1 - s][...] = t
                    at[0, :, pl.ds(pl.multiple_of(nxt * TB, TB), TB)] = t
                    first[...] += jnp.dot(
                        blocks[s][...], gb[0, pl.ds(pl.multiple_of(b * TB, TB), TB)], preferred_element_type=F32)

            @pl.when(i == 1)
            def _():
                for copy in gcopies(1):
                    copy.start()
            return 0

        lax.fori_loop(0, nb // 2, head, 0)
    for copy in gcopies(2):
        copy.start()
    xs[0] = first[:, W:].astype(BF)
    pl.semaphore_wait(barrier, 1 + 2 * (side - 1))
    send_a(0)
    acc[0] = first[:, :W]

    done = 0
    for t in range(1, K):
        with jax.named_scope("top"):
            for copy in gcopies(t + 1) if 1 < t < K - 1 else ():
                copy.start()
            for b in range(2 * t - 2, min(2 * t, nb)):
                acopy(1, b).start()
            beside = []
            for item in STEPS[t]:
                name, k = item[0].upper(), int(item[1:])
                if item[0] == name:
                    stage(name, k)
                else:
                    waits[name](k)
                    beside.append((name, k))
            turns = range(done, min(done + 2, nb)) if t > 2 else ()
            done += len(turns)
            for b in turns:
                acopy(1, b).wait()
            for copy in gcopies(t):
                copy.wait()
        with jax.named_scope("dot"):
            @pl.when(me >= 0)
            def _():
                for b in turns:
                    at[1, :, b * TB:(b + 1) * TB] = ast[b].T
                for name, k in beside:
                    works[name](k)
                res = jnp.dot(at[t // per], gb[t % 2], preferred_element_type=F32)
                acc[t % RING] = res[:, :W]
                xs[t] = res[:, W:].astype(BF)
        with jax.named_scope("end"):
            send_a(t)
            for name, k in beside:
                sends[name](k)
    for item in DRAIN:
        with jax.named_scope(item):
            stage(item[0], int(item[1:]))
    recv(7, 0, xr)
    for kind, size in zip(KINDS, (xs, sb, tb, tb, sb, xs)):
        remote(kind, 0, 0, size, size, partner).wait_send()


def write(o_ref, out_ref, sem):
    w = o_ref.shape[-1]
    per = out_ref.shape[2] // w
    blocks = out_ref.shape[0] * per

    def copy(k):
        return pltpu.make_async_copy(
            o_ref.at[k], out_ref.at[k // per, :, pl.ds(k % per * w, w)], sem.at[k])

    for k in range(blocks):
        copy(k).start()
    for k in range(blocks):
        copy(k).wait()


def solution(mesh):
    n = mesh.shape["dp"]
    side = math.isqrt(n // 2)

    def step(a, g):
        _, mats, tokens, rows = a.shape
        cols = g.shape[-1]
        K = mats * cols // (2 * W)
        quarter, piece = rows // side, rows // side // side
        o = pl.pallas_call(
            functools.partial(kernel, n, mats, tokens, rows, cols),
            out_shape=pltpu.VMEM((K, side, side, piece, 2 * W), BF),
            in_specs=[pl.BlockSpec(memory_space=pl.ANY)] * 2,
            out_specs=pl.BlockSpec(memory_space=pltpu.VMEM),
            scratch_shapes=[
                pltpu.VMEM((mats, rows, tokens), BF),
                pltpu.VMEM((tokens // TB, TB, rows), BF),
                pltpu.VMEM((rows, TB), BF),
                pltpu.VMEM((rows, TB), BF),
                pltpu.VMEM((2, tokens, 2 * W), BF),
                pltpu.VMEM((RING, rows, W), F32),
                pltpu.VMEM((rows, 2 * W), F32),
                pltpu.VMEM((K, rows, W), BF),
                pltpu.VMEM((K, rows, W), BF),
                pltpu.VMEM((K, 2, quarter, W), F32),
                pltpu.VMEM((K, 3, quarter, W), BF),
                pltpu.VMEM((K, 3, quarter, W), BF),
                pltpu.VMEM((K, side, piece, W), F32),
                pltpu.VMEM((K, 3, piece, W), BF),
                pltpu.VMEM((K, 3, piece, W), BF),
                pltpu.SemaphoreType.DMA((tokens // TB,)),
                pltpu.SemaphoreType.DMA((2, 2)),
                pltpu.SemaphoreType.DMA((2, tokens // TB)),
                pltpu.SemaphoreType.DMA((len(KINDS),)),
                pltpu.SemaphoreType.DMA((10 if NEAR else 7, K)),
                pltpu.SemaphoreType.DMA,
            ],
            name="sums",
            compiler_params=pltpu.CompilerParams(
                collective_id=0, has_side_effects=True, vmem_limit_bytes=55 * 2**20),
        )(a, g)
        o = o.reshape(K, rows, 2 * W)
        return pl.pallas_call(
            write,
            out_shape=jax.ShapeDtypeStruct((mats, rows, cols), BF),
            in_specs=[pl.BlockSpec(memory_space=pltpu.VMEM)],
            out_specs=pl.BlockSpec(memory_space=pl.ANY),
            scratch_shapes=[pltpu.SemaphoreType.DMA((K,))],
            name="write",
            compiler_params=pltpu.CompilerParams(vmem_limit_bytes=8 * 2**20),
        )(pltpu.with_memory_space_constraint(o, pltpu.VMEM))

    return jax.shard_map(
        step, mesh=mesh, in_specs=(P(("rep", "dp")), P(("rep", "dp"))), out_specs=P("rep"), check_vma=False)
```
